8 devices in a mesh: dp: 1 (over z), tp: 8 (over x, y, core).
Axes of the slice: x: 2, y: 2, z: 1, core: 2. Of those that a mesh axis runs over, the one named last changes fastest.
Arguments:
- x: bfloat16 [2048, 2048], P('dp')
- dy: bfloat16 [2048, 2048], P('dp')
- gate: bfloat16 [2048, 8192], P('dp', 'tp')
- up: bfloat16 [2048, 8192], P('dp', 'tp')
- w_gate: bfloat16 [2048, 8192], P(None, 'tp')
- w_up: bfloat16 [2048, 8192], P(None, 'tp')
- w_down: bfloat16 [8192, 2048], P('tp')
Outputs:
- output 1: bfloat16 [2048, 2048], P('dp')
- output 2: bfloat16 [2048, 8192], P('dp', 'tp')
- output 3: bfloat16 [2048, 8192], P('dp', 'tp')
- output 4: bfloat16 [8192, 2048], P(('dp', 'tp'))
All inputs are finite; a program needn't handle non-finite values.
Results may differ from the reference program's by a relative error of at most 0.012.
Values are sent between devices in bfloat16 or wider.
A program may use at most 2 GiB of HBM per device.

```python
import jax
import jax.numpy as jnp

ROWS = 2048
D = 2048
FF = 8192


def act(gate, up):
    return jax.nn.silu(gate) * up


def setup_inputs(seed: int = 0, part: int = 0) -> dict:
    kx, ky, ka, kb, kg, ku, kd = jax.random.split(jax.random.key(seed), 7)
    kx, ky, ka, kb = (jax.random.fold_in(k, part) for k in (kx, ky, ka, kb))
    drawn = {
        "x": jax.random.normal(kx, (ROWS, D), jnp.float32),
        "dy": jax.random.normal(ky, (ROWS, D), jnp.float32),
        "gate": jax.random.normal(ka, (ROWS, FF), jnp.float32),
        "up": jax.random.normal(kb, (ROWS, FF), jnp.float32),
        "w_gate": jax.random.normal(kg, (D, FF), jnp.float32) * D**-0.5,
        "w_up": jax.random.normal(ku, (D, FF), jnp.float32) * D**-0.5,
        "w_down": jax.random.normal(kd, (FF, D), jnp.float32) * FF**-0.5,
    }
    return {k: v.astype(jnp.bfloat16) for k, v in drawn.items()}


def reference(x, dy, gate, up, w_gate, w_up, w_down):
    hidden, back = jax.vjp(act, gate.astype(jnp.float32), up.astype(jnp.float32))
    d_hidden = jnp.dot(dy, w_down.T, preferred_element_type=jnp.float32)
    d_gate, d_up = (g.astype(jnp.bfloat16) for g in back(d_hidden))
    dx = jnp.dot(d_gate, w_gate.T, preferred_element_type=jnp.float32) + jnp.dot(d_up, w_up.T, preferred_element_type=jnp.float32)
    dw_gate = jnp.dot(x.T, d_gate, preferred_element_type=jnp.float32)
    dw_up = jnp.dot(x.T, d_up, preferred_element_type=jnp.float32)
    dw_down = jnp.dot(hidden.astype(jnp.bfloat16).T, dy, preferred_element_type=jnp.float32)
    return tuple(g.astype(jnp.bfloat16) for g in (dx, dw_gate, dw_up, dw_down))
```

```python
import functools

import jax
import jax.numpy as jnp
from jax import lax
from jax.experimental import pallas as pl
from jax.experimental.pallas import tpu as pltpu
from jax.sharding import PartitionSpec as P


BF, F32 = jnp.bfloat16, jnp.float32
NT = (((1,), (1,)), ((), ()))
TN = (((0,), (0,)), ((), ()))
ANY = pl.BlockSpec(memory_space=pl.ANY)
CHUNKS = (256, 512, 512, 512, 256)
Q = 256
VMEM_LIMIT = 63 * 2**20


def place():
    me = lax.axis_index("tp")
    x, y, c = me // 4, (me // 2) % 2, me % 2
    first = (1 - c) * x + c * y
    second = (1 - c) * y + c * x
    return me, x, y, c, first, second


def neighbours():
    me, x, y, c, _, _ = place()
    over_x = (1 - x) * 4 + y * 2 + c
    over_y = x * 4 + (1 - y) * 2 + c
    partner = x * 4 + y * 2 + 1 - c
    return partner, (1 - c) * over_x + c * over_y, (1 - c) * over_y + c * over_x


def dx_kernel(
    dy, gate, up, wd, wg, wu,
    dg_out, du_out, hid_out, sh_out,
    wd_v, wg_v, wu_v, dy_v, gate_v, up_v, dg_v, du_v, hid_v,
    mate_s, mate_r, keep, one_s, one_r, two_s, two_r, sh_v,
    w_sem, in_sem, out_sem, mate_ss, mate_rs, one_ss, one_rs, two_ss, two_rs, sh_sem,
):
    n = len(CHUNKS)
    starts = [sum(CHUNKS[:k]) for k in range(n)]
    _, _, _, c, a, b = place()
    partner, near, far = neighbours()

    def rows(k):
        return pl.ds(starts[k], CHUNKS[k])

    def inputs(k):
        s, size = k % 2, CHUNKS[k]
        pairs = ((dy, dy_v), (gate, gate_v), (up, up_v))
        return [
            pltpu.make_async_copy(src.at[rows(k), :], dst.at[s, pl.ds(0, size), :], in_sem.at[s, i])
            for i, (src, dst) in enumerate(pairs)
        ]

    def outputs(k):
        s, size = k % 2, CHUNKS[k]
        pairs = ((dg_v, dg_out), (du_v, du_out), (hid_v, hid_out))
        return [
            pltpu.make_async_copy(src.at[s, pl.ds(0, size), :], dst.at[rows(k), :], out_sem.at[s, i])
            for i, (src, dst) in enumerate(pairs)
        ]

    weights = [pltpu.make_async_copy(src, dst, w_sem.at[i]) for i, (src, dst) in enumerate(((wd, wd_v), (wg, wg_v), (wu, wu_v)))]

    def remote(src, dst, ss, rs, to):
        return pltpu.make_async_remote_copy(
            src_ref=src, dst_ref=dst, send_sem=ss, recv_sem=rs, device_id={"tp": to}, device_id_type=pl.DeviceIdType.MESH
        )

    def mate(k, j, half):
        blk = pl.ds(pl.multiple_of(2 * half, 2), 2)
        return remote(mate_s.at[blk, rows(k), :], mate_r.at[blk, rows(k), :], mate_ss.at[k, j], mate_rs.at[k, j], partner)

    def one(k):
        return remote(one_s.at[:, rows(k), :], one_r.at[:, rows(k), :], one_ss.at[k], one_rs.at[k], near)

    def two(k):
        return remote(two_s.at[rows(k), :], two_r.at[rows(k), :], two_ss.at[k], two_rs.at[k], far)

    def term(k, core, half):
        s, size = k % 2, CHUNKS[k]
        w = pl.ds(pl.multiple_of(core * 1024 + half * 512, 512), 512)
        return lax.dot_general(
            dg_v[s, pl.ds(0, size), :], wg_v[w, :], NT, preferred_element_type=F32
        ) + lax.dot_general(du_v[s, pl.ds(0, size), :], wu_v[w, :], NT, preferred_element_type=F32)

    def second_exchange(k):
        one(k).wait_recv()
        two_s[rows(k), :] = (keep[1 - b, rows(k), :] + one_r[1 - b, rows(k), :].astype(F32)).astype(BF)
        two(k).start()

    def finish(k):
        two(k).wait_recv()
        total = keep[b, rows(k), :] + one_r[b, rows(k), :].astype(F32) + two_r[rows(k), :].astype(F32)
        sh_v[rows(k), :] = total.astype(BF)
        pltpu.make_async_copy(sh_v.at[rows(k), :], sh_out.at[rows(k), :], sh_sem.at[k]).start()

    barrier = pltpu.get_barrier_semaphore()
    weights[0].start()
    for copy in inputs(0):
        copy.start()
    weights[1].start()
    weights[2].start()
    for peer in (partner, near, far):
        pl.semaphore_signal(barrier, inc=1, device_id={"tp": peer}, device_id_type=pl.DeviceIdType.MESH)

    for k in range(n):
        s, size = k % 2, CHUNKS[k]
        if k + 1 < n:
            for copy in inputs(k + 1):
                copy.start()
        for copy in inputs(k):
            copy.wait()
        if k == 0:
            weights[0].wait()
        if k >= 2:
            for copy in outputs(k - 2):
                copy.wait()

        def hidden_block(j, _):
            cols = pl.ds(pl.multiple_of(j * 512, 512), 512)
            dh = lax.dot_general(dy_v[s, pl.ds(0, size), :], wd_v[cols, :], NT, preferred_element_type=F32)
            g = gate_v[s, pl.ds(0, size), cols].astype(F32)
            u = up_v[s, pl.ds(0, size), cols].astype(F32)
            sg = jax.nn.sigmoid(g)
            si = g * sg
            hid_v[s, pl.ds(0, size), cols] = (si * u).astype(BF)
            du_v[s, pl.ds(0, size), cols] = (dh * si).astype(BF)
            dg_v[s, pl.ds(0, size), cols] = (dh * u * (sg * (1.0 + g * (1.0 - sg)))).astype(BF)
            return 0

        lax.fori_loop(0, 2, hidden_block, 0)
        for copy in outputs(k):
            copy.start()
        if k == 0:
            weights[1].wait()
            weights[2].wait()
            pl.semaphore_wait(barrier, 3)

        for j in range(2):
            half = (1 - b) if j == 0 else b
            t = term(k, 1 - c, half)
            mate_s[2 * half, rows(k), :] = t[:, :Q].astype(BF)
            mate_s[2 * half + 1, rows(k), :] = t[:, Q:].astype(BF)
            mate(k, j, half).start()

        if k >= 2:
            finish(k - 2)

        t = term(k, c, 1 - a)
        mate(k, 0, 1 - a).wait_recv()
        one_s[0, rows(k), :] = (t[:, :Q] + mate_r[2 * (1 - a), rows(k), :].astype(F32)).astype(BF)
        one_s[1, rows(k), :] = (t[:, Q:] + mate_r[2 * (1 - a) + 1, rows(k), :].astype(F32)).astype(BF)
        one(k).start()
        if k >= 1:
            second_exchange(k - 1)
        t = term(k, c, a)
        mate(k, 1, a).wait_recv()
        keep[0, rows(k), :] = t[:, :Q] + mate_r[2 * a, rows(k), :].astype(F32)
        keep[1, rows(k), :] = t[:, Q:] + mate_r[2 * a + 1, rows(k), :].astype(F32)

    finish(n - 2)
    second_exchange(n - 1)
    finish(n - 1)
    for k in range(n):
        for j in range(2):
            mate(k, j, (1 - b) if j == 0 else b).wait_send()
        one(k).wait_send()
        two(k).wait_send()
        pltpu.make_async_copy(sh_v.at[rows(k), :], sh_out.at[rows(k), :], sh_sem.at[k]).wait()
    for k in (n - 2, n - 1):
        for copy in outputs(k):
            copy.wait()


def dx_terms(dy, gate, up, wd, wg, wu):
    n, (m, d), f = len(CHUNKS), dy.shape, gate.shape[1]
    dma = lambda *shape: pltpu.SemaphoreType.DMA(shape)
    return pl.pallas_call(
        dx_kernel,
        out_shape=[jax.ShapeDtypeStruct((m, f), BF)] * 3 + [jax.ShapeDtypeStruct((m, Q), BF)],
        in_specs=[ANY] * 6,
        out_specs=[ANY] * 4,
        scratch_shapes=[
            pltpu.VMEM((f, d), BF), pltpu.VMEM((d, f), BF), pltpu.VMEM((d, f), BF),
            pltpu.VMEM((2, 512, d), BF), pltpu.VMEM((2, 512, f), BF), pltpu.VMEM((2, 512, f), BF),
            pltpu.VMEM((2, 512, f), BF), pltpu.VMEM((2, 512, f), BF), pltpu.VMEM((2, 512, f), BF),
            pltpu.VMEM((4, m, Q), BF), pltpu.VMEM((4, m, Q), BF), pltpu.VMEM((2, m, Q), F32),
            pltpu.VMEM((2, m, Q), BF), pltpu.VMEM((2, m, Q), BF),
            pltpu.VMEM((m, Q), BF), pltpu.VMEM((m, Q), BF), pltpu.VMEM((m, Q), BF),
            dma(3), dma(2, 3), dma(2, 3), dma(n, 2), dma(n, 2), dma(n), dma(n), dma(n), dma(n), dma(n),
        ],
        compiler_params=pltpu.CompilerParams(collective_id=0, has_side_effects=True, vmem_limit_bytes=VMEM_LIMIT),
        cost_estimate=pl.CostEstimate(flops=3 * 2 * m * d * f, bytes_accessed=50 * 2**20, transcendentals=m * f),
        name="dx_terms",
    )(dy, gate, up, wd, wg, wu)


def tn_kernel(lhs, rhs, out):
    out[...] = lax.dot_general(lhs[...], rhs[...], TN, preferred_element_type=F32).astype(BF)


def tn_matmul(lhs, rhs, block, name):
    k, m = lhs.shape
    n = rhs.shape[1]
    return pl.pallas_call(
        tn_kernel,
        grid=(m // block,),
        in_specs=[pl.BlockSpec((k, block), lambda i: (0, i)), pl.BlockSpec((k, n), lambda i: (0, 0))],
        out_specs=pl.BlockSpec((block, n), lambda i: (i, 0)),
        out_shape=jax.ShapeDtypeStruct((m, n), BF),
        compiler_params=pltpu.CompilerParams(vmem_limit_bytes=40 * 2**20),
        cost_estimate=pl.CostEstimate(flops=2 * m * n * k, bytes_accessed=2 * (m * k + k * n + m * n), transcendentals=0),
        name=name,
    )(lhs, rhs)


def gather_kernel(*refs):
    pieces, out, buf, in_sem, out_sem = refs[:-4], refs[-4], refs[-3], refs[-2], refs[-1]
    _, _, _, c, a, b = place()
    cols = []
    for flip in (0, 1):
        for da, db in ((0, 0), (0, 1), (1, 0), (1, 1)):
            ia, ib = (a + da) % 2, (b + db) % 2
            core = c if flip == 0 else 1 - c
            ja, jb = (ia, ib) if flip == 0 else (ib, ia)
            cols.append(pl.multiple_of(core * 1024 + ja * 512 + jb * Q, Q))
    loads, stores = [], []
    at = 0
    for i, piece in enumerate(pieces):
        where = i // 2, (i % 2) * 1024
        loads.append(pltpu.make_async_copy(piece, buf.at[i], in_sem.at[i]))
        stores.append(
            pltpu.make_async_copy(
                buf.at[i], out.at[pl.ds(where[1], 1024), pl.ds(cols[where[0]], Q)], out_sem.at[i]
            )
        )
    for load in loads:
        load.start()
    for load, store in zip(loads, stores):
        load.wait()
        store.start()
    for store in stores:
        store.wait()


def assemble(pieces):
    k = len(pieces)
    return pl.pallas_call(
        gather_kernel,
        out_shape=jax.ShapeDtypeStruct((2048, 2048), BF),
        in_specs=[ANY] * k,
        out_specs=ANY,
        scratch_shapes=[pltpu.VMEM((k, 1024, Q), BF), pltpu.SemaphoreType.DMA((k,)), pltpu.SemaphoreType.DMA((k,))],
        compiler_params=pltpu.CompilerParams(vmem_limit_bytes=20 * 2**20),
        name="assemble",
    )(*pieces)


def index(x, y, c):
    return x * 4 + y * 2 + c


def permutation(f):
    return [(index(x, y, c), index(*f(x, y, c))) for x in (0, 1) for y in (0, 1) for c in (0, 1)]


NEAR = permutation(lambda x, y, c: (1 - x, y, c) if c == 0 else (x, 1 - y, c))
FAR = permutation(lambda x, y, c: (x, 1 - y, c) if c == 0 else (1 - x, y, c))
MATE = permutation(lambda x, y, c: (x, y, 1 - c))


def solution(mesh):
    def step(x, dy, gate, up, w_gate, w_up, w_down):
        dg, du, hid, sh = dx_terms(dy, gate, up, w_down, w_gate, w_up)
        send = lambda v, perm: lax.ppermute(v, "tp", perm)
        h = (sh[:1024], sh[1024:])
        near = [send(h[0], NEAR), None]
        far = [None, send(h[1], FAR)]
        near[1], far[0] = send(h[1], NEAR), send(h[0], FAR)
        both = [send(near[0], FAR), send(far[1], NEAR)]
        mine = [*h, *far, *near, *both]
        theirs = [send(v, MATE) for v in mine]
        swap = [theirs[i] for i in (0, 1, 4, 5, 2, 3, 6, 7)]
        dw_down = tn_matmul(hid, dy, 256, "dw_down")
        dw_gate = tn_matmul(x, dg, 512, "dw_gate")
        dw_up = tn_matmul(x, du, 512, "dw_up")
        dx = assemble([*mine, *swap])
        return dx, dw_gate, dw_up, dw_down

    tokens, columns, rows = P("dp", None), P(None, "tp"), P("tp", None)
    return jax.shard_map(
        step,
        mesh=mesh,
        in_specs=(tokens, tokens, P("dp", "tp"), P("dp", "tp"), columns, columns, rows),
        out_specs=(tokens, P("dp", "tp"), P("dp", "tp"), P(("dp", "tp"), None)),
        check_vma=False,
    )
```

```python
import functools

import jax
import jax.numpy as jnp
from jax import lax
from jax.experimental import pallas as pl
from jax.experimental.pallas import tpu as pltpu
from jax.sharding import PartitionSpec as P


BF, F32 = jnp.bfloat16, jnp.float32
NT = (((1,), (1,)), ((), ()))
TN = (((0,), (0,)), ((), ()))
ANY = pl.BlockSpec(memory_space=pl.ANY)
IN_VMEM = pl.BlockSpec(memory_space=pltpu.VMEM)
CHUNKS = (256, 256, 512, 512, 512)
PARTS = (512, 512, 512, 512)
Q = 256
VMEM_LIMIT = 43 * 2**20


def place():
    me = lax.axis_index("tp")
    x, y, c = me // 4, (me // 2) % 2, me % 2
    first = (1 - c) * x + c * y
    second = (1 - c) * y + c * x
    return me, x, y, c, first, second


def neighbours():
    me, x, y, c, _, _ = place()
    over_x = (1 - x) * 4 + y * 2 + c
    over_y = x * 4 + (1 - y) * 2 + c
    partner = x * 4 + y * 2 + 1 - c
    return partner, (1 - c) * over_x + c * over_y, (1 - c) * over_y + c * over_x


def dx_kernel(
    dy, gate, up, wd, wg, wu,
    dg_v, du_v, hid_out, top, low, mate_top, mate_low,
    wd_v, wg_v, wu_v, dy_v, gate_v, up_v, hid_v,
    mate_s, mate_r, keep, pair, one_s, one_r, two_r,
    w_sem, in_sem, hid_sem, mate_ss, mate_rs, one_ss, one_rs, two_ss, two_rs, sh_ss, sh_rs,
):
    n, parts = len(CHUNKS), len(PARTS)
    chunks = [pl.ds(sum(CHUNKS[:k]), CHUNKS[k]) for k in range(n)]
    at = [sum(PARTS[:p]) for p in range(parts)]
    rows = [pl.ds(at[p], PARTS[p]) for p in range(parts)]
    _, _, _, c, a, b = place()
    partner, near, far = neighbours()

    def inputs(k):
        s, size = k % 2, CHUNKS[k]
        return [
            pltpu.make_async_copy(src.at[chunks[k], :], dst.at[s, pl.ds(0, size), :], in_sem.at[s, i])
            for i, (src, dst) in enumerate(((dy, dy_v), (gate, gate_v), (up, up_v)))
        ]

    def hidden_out(k):
        s = k % 2
        return pltpu.make_async_copy(hid_v.at[s, :, pl.ds(0, CHUNKS[k])], hid_out.at[:, chunks[k]], hid_sem.at[s])

    def block(core, half):
        return pl.ds(pl.multiple_of(core * 1024 + half * 512, 512), 512)

    f = wd.shape[0] // 2
    pairs = [(wd.at[:f], wd_v.at[:f]), (wd.at[f:], wd_v.at[f:])]
    for w in (block(1 - c, 1 - b), block(c, 1 - a), block(1 - c, b), block(c, a)):
        pairs += [(wg.at[w, :], wg_v.at[w, :]), (wu.at[w, :], wu_v.at[w, :])]
    weights = [pltpu.make_async_copy(src, dst, w_sem.at[i]) for i, (src, dst) in enumerate(pairs)]

    def remote(src, dst, ss, rs, to):
        return pltpu.make_async_remote_copy(
            src_ref=src, dst_ref=dst, send_sem=ss, recv_sem=rs, device_id={"tp": to}, device_id_type=pl.DeviceIdType.MESH
        )

    def mate(i, half, r):
        blk = pl.ds(pl.multiple_of(2 * half, 2), 2)
        return remote(mate_s.at[blk, r, :], mate_r.at[blk, r, :], mate_ss.at[i], mate_rs.at[i], partner)

    def one(k):
        return remote(one_s.at[:, chunks[k], :], one_r.at[:, chunks[k], :], one_ss.at[k], one_rs.at[k], near)

    def two(p):
        return remote(one_s.at[0, rows[p], :], two_r.at[rows[p], :], two_ss.at[p], two_rs.at[p], far)

    def shard(p):
        mine, theirs = ((top, mate_top), (low, mate_low))[at[p] // top.shape[0]]
        r = pl.ds(at[p] % top.shape[0], PARTS[p])
        return remote(mine.at[r, :], theirs.at[r, :], sh_ss.at[p], sh_rs.at[p], partner)

    def term(r, core, half):
        w = block(core, half)
        return lax.dot_general(dg_v[r, :], wg_v[w, :], NT, preferred_element_type=F32) + lax.dot_general(
            du_v[r, :], wu_v[w, :], NT, preferred_element_type=F32
        )

    def for_partner(i, half, r):
        t = term(r, 1 - c, half)
        mate_s[2 * half, r, :] = t[:, :Q].astype(BF)
        mate_s[2 * half + 1, r, :] = t[:, Q:].astype(BF)
        mate(i, half, r).start()

    barrier = pltpu.get_barrier_semaphore()
    for copy in (*inputs(0), weights[0]):
        copy.start()
    for peer in (partner, near, far):
        pl.semaphore_signal(barrier, inc=1, device_id={"tp": peer}, device_id_type=pl.DeviceIdType.MESH)

    def first_exchange(k):
        r, size = chunks[k], pl.ds(0, CHUNKS[k])
        mate(k, 1 - a, r).wait_recv()
        for i in range(2):
            one_s[i, r, :] = (pair[i, size, :] + mate_r[2 * (1 - a) + i, r, :].astype(F32)).astype(BF)
        one(k).start()

    for k in range(n):
        s, size, r = k % 2, pl.ds(0, CHUNKS[k]), chunks[k]
        for copy in inputs(k):
            copy.wait()
        if k >= 2:
            hidden_out(k - 2).wait()
        if k == 0:
            weights[0].wait()
            for copy in weights[1:6]:
                copy.start()
        if k + 1 < n:
            for copy in inputs(k + 1):
                copy.start()

        def hidden_block(j):
            cols = pl.ds(j * 512, 512)
            dh = lax.dot_general(dy_v[s, size, :], wd_v[cols, :], NT, preferred_element_type=F32)
            g = gate_v[s, size, cols].astype(F32)
            u = up_v[s, size, cols].astype(F32)
            sg = jax.nn.sigmoid(g)
            si = g * sg
            hid_v[s, cols, size] = (si * u).astype(BF).T
            du_v[r, cols] = (dh * si).astype(BF)
            dg_v[r, cols] = (dh * u * (sg * (1.0 + g * (1.0 - sg)))).astype(BF)

        hidden_block(0)
        if k == 0:
            weights[1].wait()
        else:
            first_exchange(k - 1)
        hidden_block(1)
        hidden_out(k).start()
        if k == 0:
            for copy in weights[2:6]:
                copy.wait()
            for copy in weights[6:]:
                copy.start()
            pl.semaphore_wait(barrier, 3)
        for_partner(k, 1 - b, r)
        t = term(r, c, 1 - a)
        pair[0, size, :] = t[:, :Q]
        pair[1, size, :] = t[:, Q:]

    for copy in weights[6:]:
        copy.wait()
    for_partner(n, b, rows[0])
    first_exchange(n - 1)
    taken = 0
    for p in range(parts):
        r, size = rows[p], pl.ds(0, PARTS[p])
        if p + 1 < parts:
            for_partner(n + p + 1, b, rows[p + 1])
        t = term(r, c, a)
        mate(n + p, a, r).wait_recv()
        pair[0, size, :] = t[:, :Q] + mate_r[2 * a, r, :].astype(F32)
        pair[1, size, :] = t[:, Q:] + mate_r[2 * a + 1, r, :].astype(F32)
        while taken < n and sum(CHUNKS[:taken]) < sum(PARTS[: p + 1]):
            one(taken).wait()
            taken += 1
        one_s[0, r, :] = (pair[1 - b, size, :] + one_r[1 - b, r, :].astype(F32)).astype(BF)
        two(p).start()
        keep[r, :] = pair[b, size, :] + one_r[b, r, :].astype(F32)
    for p in range(parts):
        r = rows[p]
        two(p).wait_recv()
        own = (top, low)[at[p] // top.shape[0]]
        total = keep[r, :] + two_r[r, :].astype(F32)
        own[pl.ds(at[p] % top.shape[0], PARTS[p]), :] = total.astype(BF)
        shard(p).start()
    for p in range(parts):
        shard(p).wait_recv()
    for k in range(n):
        if k >= n - 2:
            hidden_out(k).wait()
        mate(k, 1 - b, chunks[k]).wait_send()
    for p in range(parts):
        mate(n + p, b, rows[p]).wait_send()
        two(p).wait_send()
        shard(p).wait_send()


def dx_terms(dy, gate, up, wd, wg, wu):
    n, parts, (m, d), f = len(CHUNKS), len(PARTS), dy.shape, gate.shape[1]
    dma = lambda *shape: pltpu.SemaphoreType.DMA(shape)
    return pl.pallas_call(
        dx_kernel,
        out_shape=[jax.ShapeDtypeStruct((m, f), BF)] * 2
        + [jax.ShapeDtypeStruct((f, m), BF)]
        + [jax.ShapeDtypeStruct((m // 2, Q), BF)] * 4,
        in_specs=[ANY] * 6,
        out_specs=[IN_VMEM, IN_VMEM, ANY] + [IN_VMEM] * 4,
        scratch_shapes=[
            pltpu.VMEM((f, d), BF), pltpu.VMEM((d, f), BF), pltpu.VMEM((d, f), BF),
            pltpu.VMEM((2, 512, d), BF), pltpu.VMEM((2, 512, f), BF), pltpu.VMEM((2, 512, f), BF), pltpu.VMEM((2, f, 512), BF),
            pltpu.VMEM((4, m, Q), BF), pltpu.VMEM((4, m, Q), BF), pltpu.VMEM((m, Q), F32), pltpu.VMEM((2, 512, Q), F32),
            pltpu.VMEM((2, m, Q), BF), pltpu.VMEM((2, m, Q), BF), pltpu.VMEM((m, Q), BF),
            dma(10), dma(2, 3), dma(2), dma(n + parts), dma(n + parts), dma(n), dma(n), dma(parts), dma(parts), dma(parts), dma(parts),
        ],
        compiler_params=pltpu.CompilerParams(collective_id=0, has_side_effects=True, vmem_limit_bytes=VMEM_LIMIT),
        cost_estimate=pl.CostEstimate(flops=3 * 2 * m * d * f, bytes_accessed=28 * 2**20, transcendentals=m * f),
        name="dx_terms",
    )(dy, gate, up, wd, wg, wu)


def dw_in_kernel(x, dg, du, dwg, dwu):
    for d, out in ((dg, dwg), (du, dwu)):
        out[...] = lax.dot_general(x[...], d[...], TN, preferred_element_type=F32).astype(BF)


def dw_in(x, dg, du, block=512):
    (m, d), f = x.shape, dg.shape[1]
    return pl.pallas_call(
        dw_in_kernel,
        grid=(d // block,),
        in_specs=[pl.BlockSpec((m, block), lambda i: (0, i)), IN_VMEM, IN_VMEM],
        out_specs=[pl.BlockSpec((block, f), lambda i: (i, 0))] * 2,
        out_shape=[jax.ShapeDtypeStruct((d, f), BF)] * 2,
        compiler_params=pltpu.CompilerParams(vmem_limit_bytes=39 * 2**20),
        cost_estimate=pl.CostEstimate(flops=4 * m * d * f, bytes_accessed=2 * (m * d + 2 * d * f), transcendentals=0),
        name="dw_gate_up",
    )(x, dg, du)


def stores(pieces, out, sem):
    _, _, _, c, a, b = place()
    copies = []
    for i, (ref, half, whose, da, db) in enumerate(pieces):
        core, first, second = (1 - c, b, a) if whose else (c, a, b)
        first, second = (first + da) % 2, (second + db) % 2
        cols = pl.ds(pl.multiple_of(core * 1024 + first * 512 + second * Q, Q), Q)
        copies.append(pltpu.make_async_copy(ref, out.at[pl.ds(half * 1024, 1024), cols], sem.at[i]))
    return copies


def dw_out_kernel(tags, hid_t, dy, *refs):
    pieces, out, dx, sem = refs[: len(tags)], *refs[len(tags) :]
    copies = stores([(ref, *tag) for ref, tag in zip(pieces, tags)], dx, sem)

    @pl.when(pl.program_id(0) == 0)
    def _():
        for copy in copies:
            copy.start()

    out[...] = jnp.dot(hid_t[...], dy[...], preferred_element_type=F32).astype(BF)

    @pl.when(pl.program_id(0) == pl.num_programs(0) - 1)
    def _():
        for copy in copies:
            copy.wait()


def dw_out(hid_t, dy, pieces, block=512):
    (f, m), d = hid_t.shape, dy.shape[1]
    refs, tags = zip(*pieces)
    return pl.pallas_call(
        functools.partial(dw_out_kernel, tags),
        grid=(d // block,),
        in_specs=[IN_VMEM, pl.BlockSpec((m, block), lambda i: (0, i))] + [IN_VMEM] * len(refs),
        out_specs=[pl.BlockSpec((f, block), lambda i: (0, i)), ANY],
        out_shape=[jax.ShapeDtypeStruct((f, d), BF), jax.ShapeDtypeStruct((m, d), BF)],
        scratch_shapes=[pltpu.SemaphoreType.DMA((len(refs),))],
        compiler_params=pltpu.CompilerParams(vmem_limit_bytes=48 * 2**20),
        cost_estimate=pl.CostEstimate(flops=2 * m * d * f, bytes_accessed=2 * (m * d + d * f), transcendentals=0),
        name="dw_down",
    )(hid_t, dy, *refs)


def finish_kernel(tags, before, *refs):
    del before
    pieces, dx, sem = refs[: len(tags)], *refs[len(tags) :]
    copies = stores([(ref, *tag) for ref, tag in zip(pieces, tags)], dx, sem)
    for copy in copies:
        copy.start()
    for copy in copies:
        copy.wait()


def finish(dx, pieces):
    refs, tags = zip(*pieces)
    return pl.pallas_call(
        functools.partial(finish_kernel, tags),
        out_shape=jax.ShapeDtypeStruct(dx.shape, BF),
        in_specs=[ANY] + [IN_VMEM] * len(refs),
        out_specs=ANY,
        scratch_shapes=[pltpu.SemaphoreType.DMA((len(refs),))],
        input_output_aliases={0: 0},
        compiler_params=pltpu.CompilerParams(vmem_limit_bytes=8 * 2**20),
        name="finish",
    )(dx, *refs)


def index(x, y, c):
    return x * 4 + y * 2 + c


def permutation(f):
    return [(index(x, y, c), index(*f(x, y, c))) for x in (0, 1) for y in (0, 1) for c in (0, 1)]


NEAR = permutation(lambda x, y, c: (1 - x, y, c) if c == 0 else (x, 1 - y, c))
FAR = permutation(lambda x, y, c: (x, 1 - y, c) if c == 0 else (1 - x, y, c))
MATE = permutation(lambda x, y, c: (x, y, 1 - c))


def solution(mesh):
    def step(x, dy, gate, up, w_gate, w_up, w_down):
        dg, du, hid_t, top, low, mate_top, mate_low = dx_terms(dy, gate, up, w_down, w_gate, w_up)
        send = lambda v, perm: lax.ppermute(v, "tp", perm)
        near0, far1 = send(top, NEAR), send(low, FAR)
        near1, far0 = send(low, NEAR), send(top, FAR)
        dw_gate, dw_up = dw_in(x, dg, du)
        near0, far1, dw_gate, dw_up = lax.optimization_barrier((near0, far1, dw_gate, dw_up))
        diag = [send(near0, FAR), send(far1, NEAR)]
        mate_near0, mate_far1 = send(near0, MATE), send(far1, MATE)
        early = [(top, (0, 0, 0, 0)), (low, (1, 0, 0, 0)), (mate_top, (0, 1, 0, 0)), (mate_low, (1, 1, 0, 0))]
        early += [(near0, (0, 0, 1, 0)), (far1, (1, 0, 0, 1))]
        dw_down, dx = dw_out(hid_t, dy, early)
        near1, far0, diag[0], diag[1], dw_down, dx = lax.optimization_barrier((near1, far0, *diag, dw_down, dx))
        late = [(near1, (1, 0, 1, 0)), (far0, (0, 0, 0, 1)), (diag[0], (0, 0, 1, 1)), (diag[1], (1, 0, 1, 1))]
        late += [(send(ref, MATE), (half, 1, da, db)) for ref, (half, _, da, db) in late]
        late += [(mate_near0, (0, 1, 1, 0)), (mate_far1, (1, 1, 0, 1))]
        dx = finish(dx, late)
        return dx, dw_gate, dw_up, dw_down

    tokens, columns, rows = P("dp", None), P(None, "tp"), P("tp", None)
    return jax.shard_map(
        step,
        mesh=mesh,
        in_specs=(tokens, tokens, P("dp", "tp"), P("dp", "tp"), columns, columns, rows),
        out_specs=(tokens, P("dp", "tp"), P("dp", "tp"), P(("dp", "tp"), None)),
        check_vma=False,
    )
```
